32 devices in a mesh: row: 4 (over z), col: 8 (over y, x, core).
Axes of the slice: x: 2, y: 2, z: 4, core: 2. Of those that a mesh axis runs over, the one named last changes fastest.
Arguments:
- clean: float32 [1344, 8192], P('row', 'col'), may hold values from -6 to 6
- noise: float32 [1344, 8192], P('row', 'col'), may hold values from -6 to 6
- bucket: int32 [32], replicated, may hold values from 0 to 31
- mod_table: float32 [1, 32, 1344], replicated, may hold values from -3 to 3
- w_first: float32 [1, 1344, 1344], P(None, 'row', 'col'), may hold values from -0.15625 to 0.15625
- w_second: float32 [1, 1344, 1344], P(None, 'col', 'row'), may hold values from -0.15625 to 0.15625
Outputs:
- grad_first: float32 [1, 1344, 1344], P(None, 'row', 'col')
- grad_second: float32 [1, 1344, 1344], P(None, 'col', 'row')
The draws below stay inside these ranges and needn't reach their ends.
All inputs are finite; a program needn't handle non-finite values.
Results may differ from the reference program's by a relative error of at most 0.018.
Values may be sent and summed in bfloat16 or wider, within the bound.
No kernel may reach another device: no remote copies, remote signals or barrier semaphores. Data moves between devices by JAX's collectives and lax.ppermute only.
A program may use at most 64 MiB of HBM per device.

```python
import math
import jax
import jax.numpy as jnp
from jax import lax

WIDTH = 1344
PIX = 256
BLOCKS = 1
BUCKETS = 32
SAMPLES = 32


def place_ends(array, own_key, least, top_value):
    longest = array.shape.index(max(array.shape))
    spots = []
    for shift in (0, 1):
        where = [jax.random.randint(jax.random.fold_in(own_key, axis), (), 0, length) for axis, length in enumerate(array.shape)]
        where[longest] = (where[longest] + shift) % array.shape[longest]
        spots.append(tuple(where))
    return array.at[spots[0]].set(least).at[spots[1]].set(top_value)


def shard_levels(rng, extent, cuts, low, high):
    def one(dim, shards_of):
        heights = jax.random.uniform(jax.random.fold_in(jax.random.fold_in(rng, 6), dim), (shards_of,), jnp.float32, low / len(cuts), high / len(cuts))
        return jnp.repeat(jnp.exp(heights), extent[dim] // shards_of).reshape((-1,) + (1,) * (len(extent) - dim - 1))

    level = one(*cuts[0])
    for cut in cuts[1:]:
        level = level * one(*cut)
    return level


def scatter_about(stream_key, dims, deviation, bound, cuts=(), kind=jnp.bfloat16):
    values = jax.random.normal(stream_key, dims, jnp.float32) * deviation
    if len(cuts) > 0:
        values = shard_levels(stream_key, dims, cuts, -0.22, 0.18) * values
    return jnp.clip(values, min=-bound, max=bound).astype(kind)


def setup_inputs(seed: int = 0) -> dict:
    seeds = jax.random.split(jax.random.key(seed), 7)
    clean = scatter_about(seeds[0], (WIDTH, SAMPLES * PIX), 1.0, 6.0, ((0, 4), (1, 8)), jnp.float32)
    noise = scatter_about(seeds[1], (WIDTH, SAMPLES * PIX), 1.0, 6.0, ((0, 4), (1, 8)), jnp.float32)
    bucket = place_ends(jax.random.randint(seeds[2], (SAMPLES,), 0, BUCKETS), jax.random.fold_in(seeds[2], 1), 0, BUCKETS - 1).astype(jnp.int32)
    mod_table = scatter_about(seeds[3], (BLOCKS, BUCKETS, WIDTH), 0.3, 3.0, (), jnp.float32)
    w_first = scatter_about(seeds[4], (BLOCKS, WIDTH, WIDTH), WIDTH ** -0.5, 0.15625, ((1, 4), (2, 8)), jnp.float32)
    w_second = scatter_about(seeds[5], (BLOCKS, WIDTH, WIDTH), WIDTH ** -0.5, 0.15625, ((1, 8), (2, 4)), jnp.float32)
    return dict(clean=clean, noise=noise, bucket=bucket, mod_table=mod_table, w_first=w_first, w_second=w_second)


MIX_WEIGHT = 0.3
KEEP_COEF = (1.0 - MIX_WEIGHT) / math.sqrt((1.0 - MIX_WEIGHT) ** 2 + MIX_WEIGHT ** 2)
ADD_COEF = MIX_WEIGHT / math.sqrt((1.0 - MIX_WEIGHT) ** 2 + MIX_WEIGHT ** 2)
SILU_GAIN = 1.0 / 0.596

def noise_levels(bucket):
    return jnp.exp(-3.0 + 5.0 * (bucket.astype(jnp.float32) + 0.5) / BUCKETS)

def silu_slope(values):
    sig = jax.nn.sigmoid(values)
    return sig * (1.0 + values * (1.0 - sig))

def reference(clean, noise, bucket, mod_table, w_first, w_second):
    clean = clean.T
    noise = noise.T
    levels = jnp.repeat(noise_levels(bucket), PIX)[:, None]
    spread_root = jnp.sqrt(levels * levels + 0.25)
    state = ((clean + levels * noise) / spread_root).astype(jnp.bfloat16)
    target = clean * (2.0 * levels / spread_root) - noise * (0.5 / spread_root)
    onehot = (bucket[:, None] == jnp.arange(BUCKETS, dtype=jnp.int32)[None, :]).astype(jnp.float32)
    saved = []
    for block in range(BLOCKS):
        col_first = jnp.sqrt(lax.optimization_barrier(jnp.sum(w_first[block] * w_first[block], axis=0)) + 1.0)
        col_second = jnp.sqrt(lax.optimization_barrier(jnp.sum(w_second[block] * w_second[block], axis=0)) + 1.0)
        normed_first = (w_first[block] / col_first[None, :]).astype(jnp.bfloat16)
        normed_second = (w_second[block] / col_second[None, :]).astype(jnp.bfloat16)
        gains = jnp.dot(onehot, 1.0 + mod_table[block], precision=lax.Precision.HIGHEST, preferred_element_type=jnp.float32)
        gains = jnp.repeat(gains, PIX, axis=0)
        pre_act = jnp.dot(state, normed_first, preferred_element_type=jnp.float32)
        hidden = (jax.nn.silu(pre_act) * SILU_GAIN * gains).astype(jnp.bfloat16)
        branch = jnp.dot(hidden, normed_second, preferred_element_type=jnp.float32)
        saved.append((state, hidden, pre_act, gains, normed_first, normed_second, col_first, col_second))
        state = (KEEP_COEF * state.astype(jnp.float32) + ADD_COEF * branch).astype(jnp.bfloat16)
    grad_state = (state.astype(jnp.float32) - target) / SAMPLES
    firsts = []
    seconds = []
    for block in range(BLOCKS - 1, -1, -1):
        state_in, hidden, pre_act, gains, normed_first, normed_second, col_first, col_second = saved[block]
        dbranch = (ADD_COEF * grad_state).astype(jnp.bfloat16)
        gsecond = jnp.dot(hidden.T, dbranch, preferred_element_type=jnp.float32)
        dhidden = jnp.dot(dbranch, normed_second.T, preferred_element_type=jnp.float32)
        dpre = (dhidden * gains * silu_slope(pre_act) * SILU_GAIN).astype(jnp.bfloat16)
        gfirst = jnp.dot(state_in.T, dpre, preferred_element_type=jnp.float32)
        if block > 0:
            grad_state = KEEP_COEF * grad_state + jnp.dot(dpre, normed_first.T, preferred_element_type=jnp.float32)
        dot_first = lax.optimization_barrier(jnp.sum(w_first[block] * gfirst, axis=0))
        dot_second = lax.optimization_barrier(jnp.sum(w_second[block] * gsecond, axis=0))
        firsts.append(gfirst / col_first[None, :] - w_first[block] * (dot_first / col_first ** 3)[None, :])
        seconds.append(gsecond / col_second[None, :] - w_second[block] * (dot_second / col_second ** 3)[None, :])
    grad_first = jnp.stack(firsts[::-1], axis=0)
    grad_second = jnp.stack(seconds[::-1], axis=0)
    return (grad_first, grad_second)
```

```python
import functools
import math

import jax
import jax.numpy as jnp
from jax import lax
from jax.sharding import PartitionSpec as P

PIX = 256
BUCKETS = 32

MIX_WEIGHT = 0.3
KEEP_COEF = (1.0 - MIX_WEIGHT) / math.sqrt((1.0 - MIX_WEIGHT) ** 2 + MIX_WEIGHT**2)
ADD_COEF = MIX_WEIGHT / math.sqrt((1.0 - MIX_WEIGHT) ** 2 + MIX_WEIGHT**2)
SILU_GAIN = 1.0 / 0.596


F32 = jnp.float32
BF16 = jnp.bfloat16


def noise_levels(bucket):
    return jnp.exp(-3.0 + 5.0 * (bucket.astype(F32) + 0.5) / BUCKETS)


def swap(value, axis, bits, size):
    return lax.ppermute(value, axis, [(i, i ^ bits) for i in range(size)])


def mm(lhs, rhs, contract):
    return lax.dot_general(lhs, rhs, ((contract[:1], contract[1:]), ((), ())), preferred_element_type=F32)


def local(clean, noise, bucket, mod_table, w_first, w_second, *, rows, cols):
    row_at = lax.axis_index("row")
    col_at = lax.axis_index("col")
    samples = bucket.shape[0]
    own_rows = clean.shape[1]
    sub_rows = own_rows // rows
    part_in = clean.shape[0]
    part_hid = w_first.shape[2]
    hid_ids = list(range(0, cols, 2))

    own1 = w_first[0].T.astype(BF16)
    own2 = w_second[0].astype(BF16)
    both = jnp.stack([own1, own2])
    pieces = [both] + [swap(both, "row", k, rows) for k in range(1, rows)]
    block1 = {0: jnp.concatenate([p[0] for p in pieces], axis=1)}
    block2 = {0: jnp.concatenate([p[1] for p in pieces], axis=1)}
    if cols == 8:
        for j in (2, 4):
            block1[j] = swap(block1[0], "col", j, cols)
            block2[j] = swap(block2[0], "col", j, cols)
        block1[6] = swap(block1[4], "col", 2, cols)
        block2[6] = swap(block2[2], "col", 4, cols)
    else:
        for j in hid_ids[1:]:
            block1[j] = swap(block1[0], "col", j, cols)
            block2[j] = swap(block2[0], "col", j, cols)

    row_bucket = jnp.repeat(bucket, PIX, total_repeat_length=samples * PIX)
    own_bucket = lax.dynamic_slice(row_bucket, (col_at * own_rows,), (own_rows,))
    levels = noise_levels(own_bucket)[None, :]
    spread_root = jnp.sqrt(levels * levels + 0.25)
    state = ((clean + levels * noise) / spread_root).astype(BF16)
    target = clean * (2.0 * levels / spread_root) - noise * (0.5 / spread_root)
    rest = (KEEP_COEF * state.astype(F32) - target).astype(BF16)

    def to_rows(value):
        cut = [
            lax.dynamic_slice(value, (0, (row_at ^ k) * sub_rows), (part_in, sub_rows))
            for k in range(rows)
        ]
        return jnp.concatenate(
            cut[:1] + [swap(cut[k], "row", k, rows) for k in range(1, rows)], axis=0
        )

    def pair_up(value):
        return jnp.concatenate([value, swap(value, "col", 1, cols)], axis=1)

    state_rows = pair_up(to_rows(state))
    rest_rows = pair_up(to_rows(rest))

    def gain_cols(j, col):
        sample = (col * own_rows + row_at * sub_rows) // PIX
        picked = lax.dynamic_slice(
            mod_table[0], (bucket[sample], (col_at ^ j) * part_hid), (1, part_hid)
        )
        return jnp.broadcast_to(1.0 + picked.T, (part_hid, sub_rows))

    raw, hidden, slope, inv1 = {}, {}, {}, {}
    branch = 0.0
    square2 = 0.0
    for j in hid_ids:
        gains = jnp.concatenate([gain_cols(j, col_at), gain_cols(j, col_at ^ 1)], axis=1)
        wide = block1[j].astype(F32)
        inv1[j] = lax.rsqrt(1.0 + jnp.sum(wide * wide, axis=1, keepdims=True))
        raw[j] = mm(block1[j], state_rows, (1, 0))
        pre = raw[j] * inv1[j]
        sig = jax.nn.sigmoid(pre)
        scaled = gains * SILU_GAIN
        hidden[j] = (pre * sig * scaled).astype(BF16)
        slope[j] = sig * (1.0 + pre * (1.0 - sig)) * scaled * inv1[j]
        wide = block2[j].astype(F32)
        square2 = square2 + jnp.sum(wide * wide, axis=0)
    all2 = jnp.concatenate([block2[j] for j in hid_ids], axis=0)
    all_hidden = jnp.concatenate([hidden[j] for j in hid_ids], axis=0)
    branch = mm(all2, all_hidden, (0, 0))
    square2 = square2 + swap(square2, "col", 1, cols)
    inv2 = lax.rsqrt(1.0 + square2)
    other = jnp.concatenate([branch[:, sub_rows:], branch[:, :sub_rows]], axis=1).astype(BF16)
    branch = branch + swap(other, "col", 1, cols).astype(F32)
    scaled = branch * inv2[:, None]
    dbranch = (
        (ADD_COEF / samples) * (rest_rows.astype(F32) + ADD_COEF * scaled) * inv2[:, None]
    ).astype(BF16)
    dot2 = jnp.sum(dbranch.astype(F32) * branch, axis=1) * inv2 * inv2

    part1, part2 = {}, {}
    for j in hid_ids[::-1]:
        part2[j] = (
            mm(hidden[j], dbranch, (1, 1)) - block2[j].astype(F32) * dot2[None, :]
        ).astype(BF16)
    for j in hid_ids[::-1]:
        dpre = (mm(block2[j], dbranch, (1, 0)) * slope[j]).astype(BF16)
        dot1 = jnp.sum(dpre.astype(F32) * raw[j], axis=1, keepdims=True) * inv1[j] * inv1[j]
        part1[j] = (mm(dpre, state_rows, (1, 1)) - block1[j].astype(F32) * dot1).astype(BF16)

    def reduce_cols(part, first, second):
        if cols == 8:
            low = swap(part[first ^ second], "col", first, cols)
            near = swap(part[first], "col", first, cols)
            own = part[0].astype(F32) + near.astype(F32)
            low = (part[second].astype(F32) + low.astype(F32)).astype(BF16)
            return (own + swap(low, "col", second, cols).astype(F32)).astype(BF16)
        total = part[0].astype(F32)
        for j in hid_ids[1:]:
            total = total + swap(part[j], "col", j, cols).astype(F32)
        return total.astype(BF16)

    def reduce_rows(part):
        cut = [part[:, k * part_in : (k + 1) * part_in] for k in range(rows)]
        total = cut[0].astype(F32)
        for k in range(1, rows):
            total = total + swap(cut[k], "row", k, rows).astype(F32)
        return total

    grad_second = reduce_rows(reduce_cols(part2, 2, 4))
    grad_first = reduce_rows(reduce_cols(part1, 4, 2)).T
    return (grad_first[None], grad_second[None])


def solution(mesh):
    placed = (
        P("row", "col"),
        P("row", "col"),
        P(),
        P(),
        P(None, "row", "col"),
        P(None, "col", "row"),
    )
    return jax.shard_map(
        functools.partial(local, rows=mesh.shape["row"], cols=mesh.shape["col"]),
        mesh=mesh,
        in_specs=placed,
        out_specs=(P(None, "row", "col"), P(None, "col", "row")),
        check_vma=False,
    )
```
